16 devices in a mesh: dp: 2 (over y, z), tp: 8 (over x, core).
Axes of the slice: x: 4, y: 2, z: 1, core: 2. Of those that a mesh axis runs over, the one named last changes fastest.
The devices are a block of a 4x4x8 slice.
Arguments:
- x_in: bfloat16 [2, 128, 5120], P('dp', 'tp'), parts along dimension 0
- start_pos: int32 [2], P('dp'), parts along dimension 0
- k_cache: bfloat16 [2, 4096, 8, 128], P('dp', None, 'tp'), parts along dimension 0
- v_cache: bfloat16 [2, 4096, 8, 128], P('dp', None, 'tp'), parts along dimension 0
- attn_gain: bfloat16 [5120], replicated
- w_query: bfloat16 [5120, 32, 128], P(None, 'tp')
- w_key: bfloat16 [5120, 8, 128], P(None, 'tp')
- w_value: bfloat16 [5120, 8, 128], P(None, 'tp')
- w_out: bfloat16 [32, 128, 5120], P('tp')
- mlp_gain: bfloat16 [5120], replicated
- w_gate: bfloat16 [5120, 14336], P(None, 'tp')
- w_up: bfloat16 [5120, 14336], P(None, 'tp')
- w_down: bfloat16 [14336, 5120], P('tp')
Outputs:
- output 1: bfloat16 [2, 128, 5120], P('dp', 'tp'), parts along dimension 0
- output 2: bfloat16 [2, 4096, 8, 128], P('dp', None, 'tp'), parts along dimension 0
- output 3: bfloat16 [2, 4096, 8, 128], P('dp', None, 'tp'), parts along dimension 0
There are 2 independent parts. The reference program is written for one: setup_inputs(seed, part) draws one part's arguments, and reference() takes and returns one part's arrays. A program takes and returns all parts, laid end to end along the dimension named above; an argument that names none is the same for every part.
All inputs are finite; a program needn't handle non-finite values.
Results may differ from the reference program's by a relative error of at most 0.0147496.
Values are sent between devices in bfloat16 or wider.
A program may use at most 768 MiB of HBM per device.

```python
import jax
import jax.numpy as jnp
from jax import lax

MODEL_DIM = 5120
Q_HEADS = 32
KV_HEADS = 8
HEAD_DIM = 128
FFN_DIM = 14336
WINDOW = 4096
BATCH_ROWS = 1
CHUNK_LEN = 128
ROPE_BASE = 10000.0
NORM_EPS = 1e-5
GROUP_SIZE = Q_HEADS // KV_HEADS
QUERY_BLOCK = min(CHUNK_LEN, 128)


def setup_inputs(seed: int = 0, part: int = 0) -> dict:
    part_keys = jax.random.split(jax.random.fold_in(jax.random.key(seed), part), 6)
    shared_keys = jax.random.split(jax.random.key(seed + 1), 9)
    cache_shape = (BATCH_ROWS, WINDOW, KV_HEADS, HEAD_DIM)
    x_in = jax.random.normal(part_keys[0], (BATCH_ROWS, CHUNK_LEN, MODEL_DIM), jnp.float32)
    row_starts = jax.random.randint(part_keys[1], (BATCH_ROWS,), 0, 3 * WINDOW)
    first_start = jax.random.randint(part_keys[2], (), WINDOW, 3 * WINDOW)
    start_pos = jnp.where(jnp.arange(BATCH_ROWS) == 0, first_start, row_starts)
    k_cache = 1.5 * jax.random.normal(part_keys[3], cache_shape, jnp.float32)
    v_mean = jax.random.normal(part_keys[4], (BATCH_ROWS, 1, KV_HEADS, HEAD_DIM), jnp.float32)
    v_cache = v_mean + jax.random.normal(part_keys[5], cache_shape, jnp.float32)
    attn_gain = 1.0 + 0.25 * jax.random.normal(shared_keys[0], (MODEL_DIM,), jnp.float32)
    w_query = (1.5 * MODEL_DIM ** -0.5) * jax.random.normal(shared_keys[1], (MODEL_DIM, Q_HEADS, HEAD_DIM), jnp.float32)
    w_key = (1.5 * MODEL_DIM ** -0.5) * jax.random.normal(shared_keys[2], (MODEL_DIM, KV_HEADS, HEAD_DIM), jnp.float32)
    w_value = MODEL_DIM ** -0.5 * jax.random.normal(shared_keys[3], (MODEL_DIM, KV_HEADS, HEAD_DIM), jnp.float32)
    w_out = (Q_HEADS * HEAD_DIM) ** -0.5 * jax.random.normal(shared_keys[4], (Q_HEADS, HEAD_DIM, MODEL_DIM), jnp.float32)
    mlp_gain = 1.0 + 0.25 * jax.random.normal(shared_keys[5], (MODEL_DIM,), jnp.float32)
    w_gate = MODEL_DIM ** -0.5 * jax.random.normal(shared_keys[6], (MODEL_DIM, FFN_DIM), jnp.float32)
    w_up = MODEL_DIM ** -0.5 * jax.random.normal(shared_keys[7], (MODEL_DIM, FFN_DIM), jnp.float32)
    w_down = FFN_DIM ** -0.5 * jax.random.normal(shared_keys[8], (FFN_DIM, MODEL_DIM), jnp.float32)
    return {
        'x_in': x_in.astype(jnp.bfloat16),
        'start_pos': start_pos.astype(jnp.int32),
        'k_cache': k_cache.astype(jnp.bfloat16),
        'v_cache': v_cache.astype(jnp.bfloat16),
        'attn_gain': attn_gain.astype(jnp.bfloat16),
        'w_query': w_query.astype(jnp.bfloat16),
        'w_key': w_key.astype(jnp.bfloat16),
        'w_value': w_value.astype(jnp.bfloat16),
        'w_out': w_out.astype(jnp.bfloat16),
        'mlp_gain': mlp_gain.astype(jnp.bfloat16),
        'w_gate': w_gate.astype(jnp.bfloat16),
        'w_up': w_up.astype(jnp.bfloat16),
        'w_down': w_down.astype(jnp.bfloat16),
    }


def rms_norm(rows, gain):
    rows32 = rows.astype(jnp.float32)
    inv_rms = lax.rsqrt(jnp.mean(rows32 * rows32, axis=-1, keepdims=True) + NORM_EPS)
    return (rows32 * inv_rms * gain.astype(jnp.float32)).astype(jnp.bfloat16)


def rotate(heads_in, positions):
    inv_freq = jnp.power(ROPE_BASE, -jnp.arange(0, HEAD_DIM, 2).astype(jnp.float32) / HEAD_DIM)
    angles = positions.astype(jnp.float32)[:, None] * inv_freq[None, :]
    cos_t = jnp.cos(angles)[:, None, :]
    sin_t = jnp.sin(angles)[:, None, :]
    pairs = heads_in.reshape(heads_in.shape[0], heads_in.shape[1], HEAD_DIM // 2, 2)
    even = pairs[..., 0]
    odd = pairs[..., 1]
    turned = jnp.stack([even * cos_t - odd * sin_t, even * sin_t + odd * cos_t], axis=-1)
    return turned.reshape(heads_in.shape)


def layer_row(x_row, start, k_old, v_old, attn_gain, w_query, w_key, w_value, w_out, mlp_gain, w_gate, w_up, w_down):
    positions = start + jnp.arange(CHUNK_LEN)
    normed = rms_norm(x_row, attn_gain)
    q_lin = jnp.dot(normed, w_query.reshape(MODEL_DIM, Q_HEADS * HEAD_DIM), preferred_element_type=jnp.float32)
    k_lin = jnp.dot(normed, w_key.reshape(MODEL_DIM, KV_HEADS * HEAD_DIM), preferred_element_type=jnp.float32)
    v_lin = jnp.dot(normed, w_value.reshape(MODEL_DIM, KV_HEADS * HEAD_DIM), preferred_element_type=jnp.float32)
    queries = rotate(q_lin.reshape(CHUNK_LEN, Q_HEADS, HEAD_DIM), positions).astype(jnp.bfloat16)
    k_chunk = rotate(k_lin.reshape(CHUNK_LEN, KV_HEADS, HEAD_DIM), positions).astype(jnp.bfloat16)
    v_chunk = v_lin.astype(jnp.bfloat16).reshape(CHUNK_LEN, KV_HEADS, HEAD_DIM)
    offsets = jnp.mod(jnp.arange(WINDOW) - start, WINDOW)
    cache_valid = (start - WINDOW + offsets) >= 0
    keys = jnp.concatenate([k_old, k_chunk], axis=0).astype(jnp.float32)
    values = jnp.concatenate([v_old, v_chunk], axis=0).astype(jnp.float32)
    n_blocks = CHUNK_LEN // QUERY_BLOCK
    q_tiles = queries.reshape(n_blocks, QUERY_BLOCK, KV_HEADS, GROUP_SIZE, HEAD_DIM)

    def attend_block(tile_pair):
        q_tile, block = tile_pair
        q_ids = block * QUERY_BLOCK + jnp.arange(QUERY_BLOCK)
        cache_mask = cache_valid[None, :] & (offsets[None, :] > q_ids[:, None])
        chunk_mask = jnp.arange(CHUNK_LEN)[None, :] <= q_ids[:, None]
        mask = jnp.concatenate([cache_mask, chunk_mask], axis=1)
        scores = jnp.einsum('qkge,ske->kgqs', q_tile.astype(jnp.float32), keys) * (HEAD_DIM ** -0.5)
        scores = jnp.where(mask[None, None], scores, -jnp.inf)
        attn_probs = jax.nn.softmax(scores, axis=-1).astype(jnp.bfloat16)
        mixed = jnp.einsum('kgqs,ske->qkge', attn_probs.astype(jnp.float32), values)
        return mixed.astype(jnp.bfloat16)

    mixed = lax.map(attend_block, (q_tiles, jnp.arange(n_blocks)))
    attn_out = jnp.dot(mixed.reshape(CHUNK_LEN, Q_HEADS * HEAD_DIM), w_out.reshape(Q_HEADS * HEAD_DIM, MODEL_DIM), preferred_element_type=jnp.float32)
    hidden = (x_row.astype(jnp.float32) + attn_out).astype(jnp.bfloat16)
    mlp_rows = rms_norm(hidden, mlp_gain)
    gate = jnp.dot(mlp_rows, w_gate, preferred_element_type=jnp.float32)
    up_proj = jnp.dot(mlp_rows, w_up, preferred_element_type=jnp.float32)
    activated = (jax.nn.silu(gate) * up_proj).astype(jnp.bfloat16)
    mlp_out = jnp.dot(activated, w_down, preferred_element_type=jnp.float32)
    x_out = (hidden.astype(jnp.float32) + mlp_out).astype(jnp.bfloat16)
    slots = jnp.mod(start + jnp.arange(CHUNK_LEN), WINDOW)
    k_new = k_old.at[slots].set(k_chunk)
    v_new = v_old.at[slots].set(v_chunk)
    return x_out, k_new, v_new


def reference(x_in, start_pos, k_cache, v_cache, attn_gain, w_query, w_key, w_value, w_out, mlp_gain, w_gate, w_up, w_down):
    def one_row(row_inputs):
        x_row, start, k_old, v_old = row_inputs
        return layer_row(x_row, start, k_old, v_old, attn_gain, w_query, w_key, w_value, w_out, mlp_gain, w_gate, w_up, w_down)

    x_out, k_new, v_new = lax.map(one_row, (x_in, start_pos, k_cache, v_cache))
    return x_out, k_new, v_new
```

```python
import functools

import jax
import jax.numpy as jnp
from jax import lax
from jax.experimental import pallas as pl
from jax.experimental.pallas import tpu as pltpu
from jax.sharding import PartitionSpec as P

ROPE_BASE = 10000.0
NORM_EPS = 1e-5
MESH = pl.DeviceIdType.MESH
BF16 = jnp.bfloat16
F32 = jnp.float32
SLOT = 256

LA, LB, RA, RB, OA, OB, PMA, PMB, PLA, PLB, PRA, PRB, POA, POB = range(14)


def layer_kernel(
    n_dev, dims,
    start_ref, x_ref, kc_hbm, vc_hbm, ag_ref, wq_hbm, wk_hbm, wv_hbm, wo_hbm, mg_ref, wg_hbm, wu_hbm, wd_hbm, cos_ref, sin_ref,
    xout_ref, kch_ref, vch_ref,
    g1, g2, nbuf, mbuf, part1, part2, prec1, prec2, rel1, rel2, fin1, fin2, ssbuf, arena, wo, raw, rawf, kt, kc, vc,
    qbuf, sbuf, obuf, acc, ubuf,
    loc_sem, raw_sem, gu_sem, wd_sem,
    a1_send, a1_recv, a2_send, a2_recv, ss_send, ss_recv, d1_send, d1_recv, d2_send, d2_recv, r1_send, r1_recv, r2_send, r2_recv,
):
    D, T, TL, HD, F, W, G = dims
    n_chip = n_dev // 2
    dblk = D // n_dev
    dchip = D // n_chip
    me = lax.axis_index("tp")
    chip = lax.div(me, 2)
    core = lax.rem(me, 2)
    other = 1 - core
    right = lax.rem(chip + 1, n_chip)
    left = lax.rem(chip + n_chip - 1, n_chip)
    opp = lax.rem(chip + 2, n_chip)
    partner = 2 * chip + other
    right_dev = 2 * right + core
    left_dev = 2 * left + core
    own = me

    half_n = T // 2

    x_in = pltpu.make_async_copy(x_ref, g1.at[own], loc_sem.at[0])
    x_in.start()

    n_raw = raw_sem.shape[0]
    raw_rows = raw.shape[1]

    def raw_copy(i):
        return pltpu.make_async_copy(wq_hbm.at[pl.ds(i * raw_rows, raw_rows)], raw.at[i % 2], raw_sem.at[i])

    R_KV, R_Q = 0, D
    gu_n = 2 * F // SLOT
    gu_rows = gu_n * dchip

    def gu_base(s):
        return gu_rows * (s + 1) if s < n_chip - 1 else 0

    order = (chip, left, right, opp)

    def gu_copy(s, n):
        src = wg_hbm if n < gu_n // 2 else wu_hbm
        nn = n % (gu_n // 2)
        rows = pl.ds(pl.multiple_of(order[s] * dchip, dchip), dchip)
        return pltpu.make_async_copy(src.at[rows, pl.ds(nn * SLOT, SLOT)], arena.at[pl.ds(gu_base(s) + n * dchip, dchip)], gu_sem.at[s, n])

    wd_base = gu_rows

    def wd_copy(j):
        return pltpu.make_async_copy(wd_hbm.at[:, pl.ds(j * SLOT, SLOT)], arena.at[pl.ds(wd_base + j * F, F)], wd_sem.at[j])

    wk_copy = pltpu.make_async_copy(wk_hbm, arena.at[pl.ds(R_KV, D), pl.ds(0, HD)], loc_sem.at[1])
    wv_copy = pltpu.make_async_copy(wv_hbm, arena.at[pl.ds(R_KV, D), pl.ds(HD, HD)], loc_sem.at[2])
    kc_copy = pltpu.make_async_copy(kc_hbm, kc, loc_sem.at[3])
    vc_copy = pltpu.make_async_copy(vc_hbm, vc, loc_sem.at[4])
    wo_copy = pltpu.make_async_copy(wo_hbm, wo, loc_sem.at[5])

    raw_copy(0).start()
    raw_copy(1).start()

    barrier = pltpu.get_barrier_semaphore()
    for k in range(1, n_dev):
        pl.semaphore_signal(barrier, inc=1, device_id={"tp": lax.rem(me + k, n_dev)}, device_id_type=MESH)
    pl.semaphore_wait(barrier, n_dev - 1)

    def gather(buf, send, recv):
        rows = buf.shape[1] // 2

        def copy(block, half, sem, dev):
            view = buf.at[block, pl.ds(half * rows, rows)]
            return pltpu.make_async_remote_copy(view, view, send.at[sem], recv.at[sem], device_id={"tp": dev}, device_id_type=MESH)

        own_a = [copy(own, 0, LA, right_dev), copy(own, 0, RA, left_dev), copy(own, 0, PMA, partner)]
        own_b = [copy(own, 1, RB, left_dev), copy(own, 1, LB, right_dev), copy(own, 1, PMB, partner)]
        relay_a = copy(2 * left + core, 0, OA, right_dev)
        relay_b = copy(2 * right + core, 1, OB, left_dev)
        fwd = {
            LA: copy(2 * left + core, 0, PLA, partner), LB: copy(2 * left + core, 1, PLB, partner),
            RA: copy(2 * right + core, 0, PRA, partner), RB: copy(2 * right + core, 1, PRB, partner),
            OA: copy(2 * opp + core, 0, POA, partner), OB: copy(2 * opp + core, 1, POB, partner),
        }
        arrive = {
            LA: copy(2 * left + core, 0, LA, partner), LB: copy(2 * left + core, 1, LB, partner),
            RA: copy(2 * right + core, 0, RA, partner), RB: copy(2 * right + core, 1, RB, partner),
            OA: copy(2 * opp + core, 0, OA, partner), OB: copy(2 * opp + core, 1, OB, partner),
            PMA: copy(2 * chip + other, 0, PMA, partner), PMB: copy(2 * chip + other, 1, PMB, partner),
            PLA: copy(2 * left + other, 0, PLA, partner), PLB: copy(2 * left + other, 1, PLB, partner),
            PRA: copy(2 * right + other, 0, PRA, partner), PRB: copy(2 * right + other, 1, PRB, partner),
            POA: copy(2 * opp + other, 0, POA, partner), POB: copy(2 * opp + other, 1, POB, partner),
        }

        def on_arrival(sem):
            arrive[sem].wait_recv()
            if sem == LA:
                relay_a.start()
            if sem == RB:
                relay_b.start()
            if sem in fwd:
                fwd[sem].start()

        def drain():
            for c in own_a + own_b + [relay_a, relay_b] + list(fwd.values()):
                c.wait_send()

        return own_a, own_b, on_arrival, drain

    a1_a, a1_b, a1_arrive, a1_drain = gather(g1, a1_send, a1_recv)
    x_in.wait()
    for c in a1_a + a1_b:
        c.start()

    wk_copy.start()
    wv_copy.start()
    kc_copy.start()

    rf_rows = rawf.shape[0]

    def split_heads(i):
        raw_copy(i).wait()

        def body(j, carry):
            rawf[...] = raw[i % 2, pl.ds(pl.multiple_of(j * rf_rows, rf_rows), rf_rows), :].astype(F32)
            d0 = pl.multiple_of(i * (raw_rows // G) + j * (rf_rows // G), rf_rows // G)
            for h in range(G):
                piece = rawf[pl.ds(h, rf_rows // G, stride=G), :].astype(BF16)
                arena[pl.ds(R_Q + (h // 2) * D + d0, rf_rows // G), pl.ds((h % 2) * HD, HD)] = piece
            return carry

        lax.fori_loop(0, raw_rows // rf_rows, body, 0)
        if i + 2 < n_raw:
            raw_copy(i + 2).start()

    def norm_block(b):
        xb = g1[b].astype(F32)
        inv = lax.rsqrt(jnp.mean(xb * xb, axis=-1, keepdims=True) + NORM_EPS)
        nbuf[pl.ds(pl.multiple_of(b * TL, TL), TL), :] = (xb * inv * ag_ref[...].astype(F32)).astype(BF16)

    split_heads(0)
    vc_copy.start()
    wo_copy.start()
    split_heads(1)
    for s in range(n_chip - 1):
        for n in range(gu_n):
            gu_copy(s, n).start()
    a1_arrive(LA)
    a1_arrive(RB)
    split_heads(2)
    norm_block(own)
    a1_arrive(LB)
    a1_arrive(RA)
    split_heads(3)
    norm_block(2 * left + core)
    norm_block(2 * right + core)
    kc_copy.wait()

    def kt_body(i, carry):
        r0 = pl.multiple_of(i * HD, HD)
        kt[:, pl.ds(r0, HD)] = kc[pl.ds(r0, HD), :].astype(F32).T.astype(BF16)
        return carry

    lax.fori_loop(0, W // HD, kt_body, 0)
    a1_arrive(PMA)
    a1_arrive(PMB)
    norm_block(2 * chip + other)
    a1_arrive(PLA)
    a1_arrive(PLB)
    norm_block(2 * left + other)
    a1_arrive(PRA)
    a1_arrive(PRB)
    norm_block(2 * right + other)
    a1_arrive(OA)
    a1_arrive(OB)
    norm_block(2 * opp + core)
    a1_arrive(POA)
    a1_arrive(POB)
    norm_block(2 * opp + other)

    lane = lax.broadcasted_iota(jnp.int32, (T, HD), 1)
    is_even = lax.rem(lane, 2) == 0

    def turn(v):
        swapped = jnp.where(is_even, pltpu.roll(v, HD - 1, 1), pltpu.roll(v, 1, 1))
        return v * cos_ref[...] + swapped * sin_ref[...]

    wk_copy.wait()
    wv_copy.wait()
    kv = jnp.dot(nbuf[...], arena[pl.ds(R_KV, D), :], preferred_element_type=F32)
    kch_ref[...] = turn(kv[:, :HD]).astype(BF16)
    vch_ref[...] = kv[:, HD:].astype(BF16)
    for j in range(G // 2):
        q2 = jnp.dot(nbuf[...], arena[pl.ds(R_Q + j * D, D), :], preferred_element_type=F32)
        for hh in range(2):
            qh = turn(q2[:, hh * HD:(hh + 1) * HD]).astype(BF16)
            h = 2 * j + hh
            for u in range(2):
                qbuf[u, h * half_n:(h + 1) * half_n, :] = qh[u * half_n:(u + 1) * half_n]
    for n in range(gu_n):
        gu_copy(n_chip - 1, n).start()

    scale = HD ** -0.5
    start = start_ref[0]
    shift = lax.rem(start, W)
    rows_u = 2 * half_n
    cw = 256
    row_tok = lax.broadcasted_iota(jnp.int32, (rows_u, 1), 0)
    row_tok = jnp.where(row_tok >= half_n, row_tok - half_n, row_tok)

    def attend(u, j):
        q_u = qbuf[u, j * rows_u:(j + 1) * rows_u, :]
        q_id = row_tok + u * half_n
        s_c = lax.dot_general(q_u, kch_ref[...], (((1,), (1,)), ((), ())), preferred_element_type=F32) * scale
        s_c = jnp.where(lax.broadcasted_iota(jnp.int32, (rows_u, T), 1) <= q_id, s_c, -jnp.inf)
        top = jnp.max(s_c, axis=-1, keepdims=True)
        tops = jnp.full((rows_u, HD), -jnp.inf, F32)
        for c in range(W // cw):
            s = jnp.dot(q_u, kt[:, c * cw:(c + 1) * cw], preferred_element_type=F32) * scale
            off = c * cw + lax.broadcasted_iota(jnp.int32, (1, cw), 1) - shift
            off = jnp.where(off < 0, off + W, off)
            off = jnp.where(start - W + off >= 0, off, -1)
            s = jnp.where(off > q_id, s, -jnp.inf)
            sbuf[:, c * cw:(c + 1) * cw] = s
            for k in range(cw // HD):
                tops = jnp.maximum(tops, s[:, k * HD:(k + 1) * HD])
        top = jnp.maximum(top, jnp.max(tops, axis=-1, keepdims=True))
        e_c = jnp.exp(s_c - top)
        mass = e_c
        for c in range(W // cw):
            e = jnp.exp(sbuf[:, c * cw:(c + 1) * cw] - top)
            sbuf[:, c * cw:(c + 1) * cw] = e
            for k in range(cw // HD):
                mass = mass + e[:, k * HD:(k + 1) * HD]
        inv = 1.0 / jnp.sum(mass, axis=-1, keepdims=True)
        p_c = (e_c * inv).astype(BF16)
        p = (sbuf[...] * inv).astype(BF16)
        mixed = jnp.dot(p, vc[...], preferred_element_type=F32)
        mixed = mixed + jnp.dot(p_c, vch_ref[...], preferred_element_type=F32)
        mixed = mixed.astype(BF16)
        for hh in range(2):
            h = 2 * j + hh
            obuf[u, :, h * HD:(h + 1) * HD] = mixed[hh * half_n:(hh + 1) * half_n]

    chips = (opp, right, left, chip)

    def scatter(part, prec, rel, fin, u, d_send, d_recv, r_send, r_recv):
        rows = part.shape[3] // 2

        def view(ref, d, half):
            return ref.at[core, d, u, pl.ds(half * rows, rows)]

        def to_partner(o):
            return pltpu.make_async_remote_copy(
                part.at[other, chips[o], u], prec.at[chips[o], u], d_send.at[u, o], d_recv.at[u, o],
                device_id={"tp": partner}, device_id_type=MESH)

        def ring(src, dst, k, dev):
            return pltpu.make_async_remote_copy(src, dst, r_send.at[u, k], r_recv.at[u, k], device_id={"tp": dev}, device_id_type=MESH)

        opp_a = ring(view(part, opp, 0), rel.at[0, u], 0, right_dev)
        opp_b = ring(view(part, opp, 1), rel.at[1, u], 1, left_dev)
        right_a = ring(view(part, right, 0), fin.at[0, u], 2, right_dev)
        right_b = ring(view(part, right, 1), fin.at[1, u], 3, right_dev)
        left_a = ring(view(part, left, 0), fin.at[2, u], 4, left_dev)
        left_b = ring(view(part, left, 1), fin.at[3, u], 5, left_dev)

        def add_partner(o):
            to_partner(o).wait_recv()
            d = chips[o]
            mine = part[core, d, u].astype(F32) + prec[d, u].astype(F32)
            part[core, d, u] = mine.astype(BF16)

        def first():
            add_partner(0)
            opp_a.start()
            opp_b.start()
            add_partner(1)
            right_b.start()
            add_partner(2)
            left_a.start()

        def relay():
            opp_a.wait_recv()
            a = view(part, right, 0)
            a[...] = (a[...].astype(F32) + rel[0, u].astype(F32)).astype(BF16)
            right_a.start()
            opp_b.wait_recv()
            b = view(part, left, 1)
            b[...] = (b[...].astype(F32) + rel[1, u].astype(F32)).astype(BF16)
            left_b.start()

        def total():
            to_partner(3).wait_recv()
            for c in (right_a, right_b, left_a, left_b):
                c.wait_recv()
            mine = part[core, chip, u].astype(F32) + prec[chip, u].astype(F32)
            out = []
            for half in range(2):
                sl = slice(half * rows, (half + 1) * rows)
                out.append(mine[sl] + fin[half, u].astype(F32) + fin[2 + half, u].astype(F32))
            return out

        def drain():
            for o in range(4):
                to_partner(o).wait_send()
            for c in (opp_a, opp_b, right_a, right_b, left_a, left_b):
                c.wait_send()

        return to_partner, first, relay, total, drain

    rs1 = [scatter(part1, prec1, rel1, fin1, u, d1_send, d1_recv, r1_send, r1_recv) for u in range(2)]
    n_jj = dchip // SLOT

    def project_out(u):
        o_u = obuf[u]
        for o in range(4):
            d = chips[o]
            for jj in range(n_jj):
                cols = pl.ds(pl.multiple_of(d * dchip + jj * SLOT, SLOT), SLOT)
                res = jnp.dot(o_u, wo[:, cols], preferred_element_type=F32).astype(BF16)
                for k in range(SLOT // HD):
                    c0 = jj * SLOT + k * HD
                    part1[c0 // dblk, d, u, :, c0 % dblk:c0 % dblk + HD] = res[:, k * HD:(k + 1) * HD]
            rs1[u][0](o).start()

    my_cols = pl.ds(pl.multiple_of(me * dblk, 128), dblk)
    a2_a, a2_b, a2_arrive, a2_drain = gather(g2, a2_send, a2_recv)

    def hidden_rows(u):
        per = half_n // TL
        hb = []
        for half, sums in enumerate(rs1[u][3]()):
            xs = jnp.concatenate([g1[u * per + half * (per // 2) + i, :, my_cols] for i in range(per // 2)], axis=0)
            hid = (xs.astype(F32) + sums).astype(BF16)
            g2[own, u * half_n + half * (half_n // 2):u * half_n + (half + 1) * (half_n // 2), :] = hid
            h32 = hid.astype(F32)
            hb.append(jnp.sum(h32 * h32, axis=-1, keepdims=True))
        return hb

    vc_copy.wait()
    attend(0, 0)
    attend(0, 1)
    wo_copy.wait()
    project_out(0)
    attend(1, 0)
    rs1[0][1]()
    attend(1, 1)
    rs1[0][2]()
    project_out(1)
    rs1[1][1]()
    ss = hidden_rows(0)
    for c in a2_a:
        c.start()
    rs1[1][2]()
    ss = ss + hidden_rows(1)
    col = jnp.concatenate(ss, axis=0)
    row = jnp.broadcast_to(col, (T, T)).T[0:8]
    ssbuf[own] = row

    def ss_copy(src, k):
        dev = lax.rem(me + k, n_dev)
        return pltpu.make_async_remote_copy(ssbuf.at[src], ssbuf.at[src], ss_send.at[k - 1], ss_recv.at[k - 1], device_id={"tp": dev}, device_id_type=MESH)

    for c in a2_b:
        c.start()
    for k in range(1, n_dev):
        ss_copy(own, k).start()
    for k in range(1, n_dev):
        ss_copy(lax.rem(me + n_dev - k, n_dev), k).wait_recv()
    tot = ssbuf[0]
    for k in range(1, n_dev):
        tot = tot + ssbuf[k]
    inv_row = lax.rsqrt(tot[0:1] * (1.0 / D) + NORM_EPS)
    inv = jnp.broadcast_to(inv_row, (T, T)).T[:, 0:1]

    def gate_up(s):
        d = order[s]
        for c in range(2):
            b = 2 * d + c
            mbuf[:, c * dblk:(c + 1) * dblk] = (g2[b].astype(F32) * inv * mg_ref[b].astype(F32)).astype(BF16)
        for n in range(gu_n):
            gu_copy(s, n).wait()
            part = jnp.dot(mbuf[...], arena[gu_base(s) + n * dchip:gu_base(s) + (n + 1) * dchip, :], preferred_element_type=F32)
            if s:
                part = acc[:, n * SLOT:(n + 1) * SLOT] + part
            acc[:, n * SLOT:(n + 1) * SLOT] = part

    a2_arrive(PMA)
    a2_arrive(LA)
    a2_arrive(RB)
    a2_arrive(PMB)
    gate_up(0)
    wd_half = wd_sem.shape[0] // 2
    for j in range(wd_half):
        wd_copy(j).start()
    for s in (RA, LB, PLA, PLB):
        a2_arrive(s)
    gate_up(1)
    for j in range(wd_half, 2 * wd_half):
        wd_copy(j).start()
    a2_arrive(OA)
    a2_arrive(OB)
    a2_arrive(PRA)
    a2_arrive(PRB)
    gate_up(2)
    a2_arrive(POA)
    a2_arrive(POB)
    gate_up(3)
    half_g = gu_n // 2
    for n in range(half_g):
        gate = acc[:, n * SLOT:(n + 1) * SLOT]
        up = acc[:, (half_g + n) * SLOT:(half_g + n + 1) * SLOT]
        ubuf[:, n * SLOT:(n + 1) * SLOT] = (gate * (1.0 / (1.0 + jnp.exp(-gate))) * up).astype(BF16)

    n_q = n_chip
    rs2 = [scatter(part2, prec2, rel2, fin2, q, d2_send, d2_recv, r2_send, r2_recv) for q in range(n_q)]

    def down(q):
        for jj in range(n_jj):
            j = q * n_jj + jj
            wd_copy(j).wait()
            res = jnp.dot(ubuf[...], arena[wd_base + j * F:wd_base + (j + 1) * F, :], preferred_element_type=F32).astype(BF16)
            for b in range(n_dev):
                part2[b % 2, b // 2, q, :, jj * SLOT:(jj + 1) * SLOT] = res[b * TL:(b + 1) * TL]
        for o in range(4):
            rs2[q][0](o).start()

    def finish(q):
        sums = jnp.concatenate(rs2[q][3](), axis=0)
        tok = pl.ds(pl.multiple_of(me * TL, TL), TL)
        hid = jnp.concatenate([g2[2 * q + c, tok, :] for c in range(2)], axis=1)
        xout_ref[:, q * dchip:(q + 1) * dchip] = (hid.astype(F32) + sums).astype(BF16)

    down(0)
    down(1)
    rs2[0][1]()
    down(2)
    rs2[1][1]()
    down(3)
    rs2[2][1]()
    rs2[0][2]()
    rs2[3][1]()
    rs2[1][2]()
    rs2[2][2]()
    rs2[3][2]()
    for q in range(n_q):
        finish(q)

    a1_drain()
    a2_drain()
    for k in range(1, n_dev):
        ss_copy(own, k).wait_send()
    for r in rs1 + rs2:
        r[4]()


def write_chunk(cache, chunk, start_pos):
    window = cache.shape[1]
    chunk_len = chunk.shape[1]

    def one_row(old_rows, new_rows, start):
        filler = jnp.zeros((window - chunk_len,) + new_rows.shape[1:], new_rows.dtype)
        doubled = jnp.concatenate([new_rows, filler, new_rows, filler], axis=0)
        shift = jnp.mod(start, window)
        placed = lax.dynamic_slice_in_dim(doubled, window - shift, window, axis=0)
        offsets = jnp.mod(jnp.arange(window) - start, window)
        return jnp.where((offsets < chunk_len)[:, None, None], placed, old_rows)

    return jax.vmap(one_row)(cache, chunk, start_pos)


def solution(mesh):
    row_spec = P('dp', 'tp', None)
    cache_spec = P('dp', None, 'tp', None)
    head_cols = P(None, 'tp', None)
    in_specs = (row_spec, P('dp'), cache_spec, cache_spec, P(), head_cols, head_cols, head_cols, P('tp', None, None), P(), P(None, 'tp'), P(None, 'tp'), P('tp', None))
    out_specs = (row_spec, cache_spec, cache_spec)
    n_dev = mesh.shape['tp']

    def local_layer(x_in, start_pos, k_cache, v_cache, attn_gain, w_query, w_key, w_value, w_out, mlp_gain, w_gate, w_up, w_down):
        _, TL, D = x_in.shape
        W, HD = k_cache.shape[1], k_cache.shape[3]
        G = w_query.shape[1]
        F = w_gate.shape[1]
        T = TL * n_dev
        n_chip = n_dev // 2
        dblk, dchip = D // n_dev, D // n_chip
        inv_freq = jnp.power(ROPE_BASE, -jnp.arange(0, HD, 2).astype(F32) / HD)
        positions = start_pos[0] + jnp.arange(T)
        angles = positions.astype(F32)[:, None] * jnp.repeat(inv_freq, 2)[None, :]
        sign = jnp.where(jnp.arange(HD) % 2 == 0, -1.0, 1.0).astype(F32)
        cos_t = jnp.cos(angles)
        sin_t = jnp.sin(angles) * sign

        vmem = pl.BlockSpec(memory_space=pltpu.VMEM)
        hbm = pl.BlockSpec(memory_space=pl.ANY)
        smem = pl.BlockSpec(memory_space=pltpu.SMEM)
        gu_n = 2 * F // SLOT
        V = pltpu.VMEM
        dma = pltpu.SemaphoreType.DMA
        n_raw = 4
        raw_rows = D * G // n_raw
        half = T // 2
        scratch = [
            V((n_dev, TL, D), BF16), V((n_dev, T, dblk), BF16), V((T, D), BF16), V((T, dchip), BF16),
            V((2, n_chip, 2, half, dblk), BF16), V((2, n_chip, n_chip, TL, dchip), BF16),
            V((n_chip, 2, half, dblk), BF16), V((n_chip, n_chip, TL, dchip), BF16),
            V((2, 2, half // 2, dblk), BF16), V((2, n_chip, TL // 2, dchip), BF16),
            V((4, 2, half // 2, dblk), BF16), V((4, n_chip, TL // 2, dchip), BF16),
            V((n_dev, 8, T), F32),
            V((n_chip * gu_n * dchip, SLOT), BF16), V((G * HD, D), BF16),
            V((2, raw_rows, HD), BF16), V((512, HD), F32),
            V((HD, W), BF16), V((W, HD), BF16), V((W, HD), BF16),
            V((2, G * half, HD), BF16), V((2 * half, W), F32), V((2, half, G * HD), BF16),
            V((T, 2 * F), F32), V((T, F), BF16),
            dma((6,)), dma((n_raw,)), dma((n_chip, gu_n)), dma((D // SLOT,)),
            dma((14,)), dma((14,)), dma((14,)), dma((14,)), dma((n_dev - 1,)), dma((n_dev - 1,)),
            dma((2, 4)), dma((2, 4)), dma((n_chip, 4)), dma((n_chip, 4)),
            dma((2, 6)), dma((2, 6)), dma((n_chip, 6)), dma((n_chip, 6)),
        ]
        x_out, k_chunk, v_chunk = pl.pallas_call(
            functools.partial(layer_kernel, n_dev, (D, T, TL, HD, F, W, G)),
            out_shape=[jax.ShapeDtypeStruct((TL, D), BF16), jax.ShapeDtypeStruct((T, HD), BF16), jax.ShapeDtypeStruct((T, HD), BF16)],
            in_specs=[smem, hbm, hbm, hbm, vmem, hbm, hbm, hbm, hbm, vmem, hbm, hbm, hbm, vmem, vmem],
            out_specs=[vmem, vmem, vmem],
            scratch_shapes=scratch,
            compiler_params=pltpu.CompilerParams(collective_id=0, has_side_effects=True, vmem_limit_bytes=67043328),
            name="layer",
        )(
            start_pos, x_in[0], k_cache.reshape(W, HD), v_cache.reshape(W, HD), attn_gain.reshape(1, D),
            w_query.reshape(D * G, HD), w_key.reshape(D, HD), w_value.reshape(D, HD), w_out.reshape(G * HD, D),
            mlp_gain.reshape(n_dev, 1, dblk), w_gate, w_up, w_down, cos_t, sin_t,
        )
        k_chunk = k_chunk.reshape(1, T, 1, HD)
        v_chunk = v_chunk.reshape(1, T, 1, HD)
        return x_out[None], write_chunk(k_cache, k_chunk, start_pos), write_chunk(v_cache, v_chunk, start_pos)

    return jax.shard_map(local_layer, mesh=mesh, in_specs=in_specs, out_specs=out_specs, check_vma=False)
```

```python
import functools

import jax
import jax.numpy as jnp
import numpy as np
from jax import lax
from jax.experimental import pallas as pl
from jax.experimental.pallas import tpu as pltpu
from jax.sharding import PartitionSpec as P

ROPE_BASE = 10000.0
NORM_EPS = 1e-5
MESH = pl.DeviceIdType.MESH
BF16 = jnp.bfloat16
F32 = jnp.float32
SLOT = 512
Q_COLS = 1024
scope = jax.named_scope

LA, LB, RA, RB, OA, OB, PMA, PMB, PLA, PLB, PRA, PRB, POA, POB = range(14)


def layer_kernel(
    n_dev, dims,
    start_ref, x_ref, kc_hbm, vc_hbm, ag_ref, wq_hbm, wk_hbm, wv_hbm, wo_hbm, mg_ref, wg_hbm, wu_hbm, wd_hbm, freq_ref,
    xout_ref, kn_hbm, vn_hbm,
    g1, g2, nbuf, mbuf, part1, part2, prec1, prec2, rel1, rel2, fin1, fin2, ssbuf, arena, wo, rawf, kt, kc, vc,
    qbuf, sbuf, obuf, acc, ubuf, kch_ref, vch_ref, again, mgain, cos_ref, sin_ref,
    loc_sem, raw_sem, kv_sem, gu_sem, wd_sem,
    a1_send, a1_recv, a2_send, a2_recv, ss_send, ss_recv, d1_send, d1_recv, d2_send, d2_recv, r1_send, r1_recv, r2_send, r2_recv,
):
    D, T, TL, HD, F, W, G = dims
    n_chip = n_dev // 2
    dblk = D // n_dev
    dchip = D // n_chip
    me = lax.axis_index("tp")
    chip = lax.div(me, 2)
    core = lax.rem(me, 2)
    other = 1 - core
    right = lax.rem(chip + 1, n_chip)
    left = lax.rem(chip + n_chip - 1, n_chip)
    opp = lax.rem(chip + 2, n_chip)
    partner = 2 * chip + other
    right_dev = 2 * right + core
    left_dev = 2 * left + core
    own = me

    half_n = T // 2

    x_in = pltpu.make_async_copy(x_ref, g1.at[own], loc_sem.at[0])
    x_in.start()

    gu_n = 2 * F // SLOT
    gu_rows = gu_n * dchip
    order = (chip, left, right, opp)

    def gu_base(s):
        return gu_rows * (s + 1) if s < n_chip - 1 else 0

    def gu_start(s):
        rows = pl.ds(pl.multiple_of(order[s] * dchip, dchip), dchip)
        for src, first in ((wg_hbm, 0), (wu_hbm, F)):
            c0 = 0
            while c0 < F:
                at = first + c0
                wide = min(SLOT - at % SLOT, F - c0)
                dst = arena.at[pl.ds(gu_base(s) + at // SLOT * dchip, dchip), pl.ds(at % SLOT, wide)]
                pltpu.make_async_copy(src.at[rows, pl.ds(c0, wide)], dst, gu_sem.at[s]).start(priority=1)
                c0 += wide

    def gu_wait(s):
        region = arena.at[pl.ds(gu_base(s), gu_rows)]
        pltpu.make_async_copy(region, region, gu_sem.at[s]).wait()

    wd_base = gu_rows
    wd_n = D // SLOT

    def wd_copy(j):
        return pltpu.make_async_copy(wd_hbm.at[:, pl.ds(j * SLOT, SLOT)], arena.at[pl.ds(wd_base + j * F, F)], wd_sem.at[j])

    n_raw = SLOT // HD
    raw_rows = D * G // n_raw
    raw_base = gu_base(n_chip - 2)

    def raw_view(i):
        return arena.at[pl.ds(raw_base, raw_rows), pl.ds(i * HD, HD)]

    def raw_copy(i):
        return pltpu.make_async_copy(wq_hbm.at[pl.ds(i * raw_rows, raw_rows)], raw_view(i), raw_sem.at[i])

    kv_rows = pl.ds(D, D // 2)
    kv_copies = [
        pltpu.make_async_copy(src.at[pl.ds(half * (D // 2), D // 2)], arena.at[kv_rows, pl.ds((2 * half + i) * HD, HD)], kv_sem.at[2 * half + i])
        for half in range(2) for i, src in enumerate((wk_hbm, wv_hbm))
    ]
    kc_copy = pltpu.make_async_copy(kc_hbm, kc, loc_sem.at[1])
    vc_copy = pltpu.make_async_copy(vc_hbm, vc, loc_sem.at[2])
    wo_copy = pltpu.make_async_copy(wo_hbm, wo, loc_sem.at[3])

    for i in range(n_raw):
        raw_copy(i).start()
    kc_copy.start()
    for c in kv_copies:
        c.start()
    vc_copy.start()
    wo_copy.start(priority=1)
    for s in range(n_chip - 2):
        gu_start(s)

    barrier = pltpu.get_barrier_semaphore()
    for k in range(1, n_dev):
        pl.semaphore_signal(barrier, inc=1, device_id={"tp": lax.rem(me + k, n_dev)}, device_id_type=MESH)
    pl.semaphore_wait(barrier, n_dev - 1)

    def gather(buf, send, recv):
        rows = buf.shape[1] // 2

        def copy(block, half, sem, dev):
            view = buf.at[block, pl.ds(half * rows, rows)]
            return pltpu.make_async_remote_copy(view, view, send.at[sem], recv.at[sem], device_id={"tp": dev}, device_id_type=MESH)

        own_a = [copy(own, 0, LA, right_dev), copy(own, 0, RA, left_dev), copy(own, 0, PMA, partner)]
        own_b = [copy(own, 1, RB, left_dev), copy(own, 1, LB, right_dev), copy(own, 1, PMB, partner)]
        relay_a = copy(2 * left + core, 0, OA, right_dev)
        relay_b = copy(2 * right + core, 1, OB, left_dev)
        fwd = {
            LA: copy(2 * left + core, 0, PLA, partner), LB: copy(2 * left + core, 1, PLB, partner),
            RA: copy(2 * right + core, 0, PRA, partner), RB: copy(2 * right + core, 1, PRB, partner),
            OA: copy(2 * opp + core, 0, POA, partner), OB: copy(2 * opp + core, 1, POB, partner),
        }
        arrive = {
            LA: copy(2 * left + core, 0, LA, partner), LB: copy(2 * left + core, 1, LB, partner),
            RA: copy(2 * right + core, 0, RA, partner), RB: copy(2 * right + core, 1, RB, partner),
            OA: copy(2 * opp + core, 0, OA, partner), OB: copy(2 * opp + core, 1, OB, partner),
            PMA: copy(2 * chip + other, 0, PMA, partner), PMB: copy(2 * chip + other, 1, PMB, partner),
            PLA: copy(2 * left + other, 0, PLA, partner), PLB: copy(2 * left + other, 1, PLB, partner),
            PRA: copy(2 * right + other, 0, PRA, partner), PRB: copy(2 * right + other, 1, PRB, partner),
            POA: copy(2 * opp + other, 0, POA, partner), POB: copy(2 * opp + other, 1, POB, partner),
        }

        def on_arrival(sem):
            arrive[sem].wait_recv()
            if sem == LA:
                relay_a.start()
            if sem == RB:
                relay_b.start()
            if sem in fwd:
                fwd[sem].start()

        def drain():
            for c in own_a + own_b + [relay_a, relay_b] + list(fwd.values()):
                c.wait_send()

        return own_a, own_b, on_arrival, drain

    a1_a, a1_b, a1_arrive, a1_drain = gather(g1, a1_send, a1_recv)
    x_in.wait()
    for c in (a1_a[0], a1_b[0], a1_b[1], a1_a[1], a1_a[2], a1_b[2]):
        c.start()


    rf_rows = rawf.shape[0]

    def split_heads(i):
        raw_copy(i).wait()

        def body(j, carry):
            rawf[...] = arena[pl.ds(raw_base + pl.multiple_of(j * rf_rows, rf_rows), rf_rows), i * HD:(i + 1) * HD].astype(F32)
            d0 = pl.multiple_of(i * (raw_rows // G) + j * (rf_rows // G), rf_rows // G)
            for h in range(G):
                arena[pl.ds(d0, rf_rows // G), h * HD:(h + 1) * HD] = rawf[pl.ds(h, rf_rows // G, stride=G), :].astype(BF16)
            return carry

        lax.fori_loop(0, raw_rows // rf_rows, body, 0)

    again[...] = ag_ref[...].astype(F32)
    mgain[...] = mg_ref[...].astype(F32)

    def norm_block(b):
        xb = g1[b].astype(F32)
        inv = lax.rsqrt(jnp.mean(xb * xb, axis=-1, keepdims=True) + NORM_EPS)
        gain = jnp.concatenate([again[i:i + 1, :] for i in range(D // HD)], axis=1)
        nbuf[pl.ds(pl.multiple_of(b * TL, TL), TL), :] = (xb * inv * gain).astype(BF16)

    kt_rows = 4 * HD

    def kt_body(i, carry):
        r0 = pl.multiple_of(i * kt_rows, kt_rows)
        kt[:, pl.ds(r0, kt_rows)] = kc[pl.ds(r0, kt_rows), :].astype(F32).T.astype(BF16)
        return carry

    lane = lax.broadcasted_iota(jnp.int32, (T, HD), 1)
    is_even = lax.rem(lane, 2) == 0

    with scope("split01"):
        split_heads(0)
        split_heads(1)
        norm_block(own)
    with scope("a1_first"):
        a1_arrive(LA)
        a1_arrive(RB)
    with scope("angles"):
        angles = (start_ref[0] + lax.broadcasted_iota(jnp.int32, (T, HD), 0)).astype(F32) * freq_ref[...]
        cos_ref[...] = jnp.cos(angles)
        sin_t = jnp.sin(angles)
        sin_ref[...] = jnp.where(is_even, -sin_t, sin_t)
    with scope("split23"):
        split_heads(2)
        split_heads(3)
        gu_start(n_chip - 2)
    with scope("a1_second"):
        a1_arrive(LB)
        a1_arrive(RA)
    with scope("norm3"):
        norm_block(2 * left + core)
        norm_block(2 * right + core)
    with scope("kt"):
        kc_copy.wait()
        lax.fori_loop(0, W // kt_rows, kt_body, 0)
    with scope("a1_near"):
        a1_arrive(PMA)
        a1_arrive(PMB)
        norm_block(2 * chip + other)
        a1_arrive(PLA)
        a1_arrive(PLB)
        norm_block(2 * left + other)
        a1_arrive(PRA)
        a1_arrive(PRB)
        norm_block(2 * right + other)
    with scope("a1_far"):
        a1_arrive(OA)
        a1_arrive(OB)
        norm_block(2 * opp + core)
        a1_arrive(POA)
        a1_arrive(POB)
        norm_block(2 * opp + other)

    def turn(v):
        swapped = jnp.where(is_even, pltpu.roll(v, HD - 1, 1), pltpu.roll(v, 1, 1))
        return v * cos_ref[...] + swapped * sin_ref[...]

    with scope("qkv"):
        for c in kv_copies:
            c.wait()
        kv = jnp.dot(nbuf[:, :D // 2], arena[kv_rows, 0:2 * HD], preferred_element_type=F32)
        kv = kv + jnp.dot(nbuf[:, D // 2:], arena[kv_rows, 2 * HD:4 * HD], preferred_element_type=F32)
        kch_ref[...] = turn(kv[:, :HD]).astype(BF16)
        vch_ref[...] = kv[:, HD:].astype(BF16)
        q_all = jnp.dot(nbuf[...], arena[pl.ds(0, D), :], preferred_element_type=F32)
        for h in range(G):
            qh = turn(q_all[:, h * HD:(h + 1) * HD]).astype(BF16)
            for u in range(2):
                qbuf[u, h * half_n:(h + 1) * half_n, :] = qh[u * half_n:(u + 1) * half_n]
        gu_start(n_chip - 1)

    scale = HD ** -0.5
    start = start_ref[0]
    shift = lax.rem(start, W)
    rows_u = 2 * half_n
    cw = 512
    row_tok = lax.broadcasted_iota(jnp.int32, (rows_u, 1), 0)
    row_tok = jnp.where(row_tok >= half_n, row_tok - half_n, row_tok)

    def attend(u, j):
        q_u = qbuf[u, j * rows_u:(j + 1) * rows_u, :]
        q_id = row_tok + u * half_n
        s_c = lax.dot_general(q_u, kch_ref[...], (((1,), (1,)), ((), ())), preferred_element_type=F32) * scale
        s_c = jnp.where(lax.broadcasted_iota(jnp.int32, (rows_u, T), 1) <= q_id, s_c, -jnp.inf)
        top = jnp.max(s_c, axis=-1, keepdims=True)
        tops = jnp.full((rows_u, HD), -jnp.inf, F32)
        for c in range(W // cw):
            s = jnp.dot(q_u, kt[:, c * cw:(c + 1) * cw], preferred_element_type=F32) * scale
            off = c * cw + lax.broadcasted_iota(jnp.int32, (1, cw), 1) - shift
            off = jnp.where(off < 0, off + W, off)
            off = jnp.where(start - W + off >= 0, off, -1)
            s = jnp.where(off > q_id, s, -jnp.inf)
            sbuf[:, c * cw:(c + 1) * cw] = s
            for k in range(cw // HD):
                tops = jnp.maximum(tops, s[:, k * HD:(k + 1) * HD])
        top = jnp.maximum(top, jnp.max(tops, axis=-1, keepdims=True))
        e_c = jnp.exp(s_c - top)
        mass = e_c
        for c in range(W // cw):
            e = jnp.exp(sbuf[:, c * cw:(c + 1) * cw] - top)
            sbuf[:, c * cw:(c + 1) * cw] = e
            for k in range(cw // HD):
                mass = mass + e[:, k * HD:(k + 1) * HD]
        inv = 1.0 / jnp.sum(mass, axis=-1, keepdims=True)
        p_c = (e_c * inv).astype(BF16)
        p = (sbuf[...] * inv).astype(BF16)
        mixed = jnp.dot(p, vc[...], preferred_element_type=F32)
        mixed = mixed + jnp.dot(p_c, vch_ref[...], preferred_element_type=F32)
        mixed = mixed.astype(BF16)
        for hh in range(2):
            h = 2 * j + hh
            obuf[u, :, h * HD:(h + 1) * HD] = mixed[hh * half_n:(hh + 1) * half_n]

    def new_cache(cache, chunk_ref, out_hbm, sem):
        token = lax.broadcasted_iota(jnp.int32, (T, T), 0) - lax.rem(start, T)
        token = jnp.where(token < 0, token + T, token)
        pick = jnp.where(token == lax.broadcasted_iota(jnp.int32, (T, T), 1), 1.0, 0.0).astype(BF16)
        placed = jnp.dot(pick, chunk_ref[...], preferred_element_type=F32)

        def body(i, carry):
            rows = pl.ds(pl.multiple_of(i * T, T), T)
            off = i * T + lax.broadcasted_iota(jnp.int32, (T, 1), 0) - shift
            off = jnp.where(off < 0, off + W, off)
            cache[rows, :] = jnp.where(off < T, placed, cache[rows, :].astype(F32)).astype(BF16)
            return carry

        lax.fori_loop(0, W // T, body, 0)
        copy = pltpu.make_async_copy(cache, out_hbm, loc_sem.at[sem])
        copy.start()
        return copy

    chips = (opp, right, left, chip)

    def scatter(part, prec, rel, fin, u, d_send, d_recv, r_send, r_recv):
        rows = part.shape[3] // 2

        def view(ref, d, half):
            return ref.at[core, d, u, pl.ds(half * rows, rows)]

        def to_partner(o):
            return pltpu.make_async_remote_copy(
                part.at[other, chips[o], u], prec.at[chips[o], u], d_send.at[u, o], d_recv.at[u, o],
                device_id={"tp": partner}, device_id_type=MESH)

        def ring(src, dst, k, dev):
            return pltpu.make_async_remote_copy(src, dst, r_send.at[u, k], r_recv.at[u, k], device_id={"tp": dev}, device_id_type=MESH)

        opp_a = ring(view(part, opp, 0), rel.at[0, u], 0, right_dev)
        opp_b = ring(view(part, opp, 1), rel.at[1, u], 1, left_dev)
        right_a = ring(view(part, right, 0), fin.at[0, u], 2, right_dev)
        right_b = ring(view(part, right, 1), fin.at[1, u], 3, right_dev)
        left_a = ring(view(part, left, 0), fin.at[2, u], 4, left_dev)
        left_b = ring(view(part, left, 1), fin.at[3, u], 5, left_dev)

        def add_partner(o):
            to_partner(o).wait_recv()
            d = chips[o]
            mine = part[core, d, u].astype(F32) + prec[d, u].astype(F32)
            part[core, d, u] = mine.astype(BF16)

        def first():
            add_partner(0)
            opp_a.start()
            opp_b.start()
            add_partner(1)
            right_b.start()
            add_partner(2)
            left_a.start()

        def relay():
            opp_a.wait_recv()
            a = view(part, right, 0)
            a[...] = (a[...].astype(F32) + rel[0, u].astype(F32)).astype(BF16)
            right_a.start()
            opp_b.wait_recv()
            b = view(part, left, 1)
            b[...] = (b[...].astype(F32) + rel[1, u].astype(F32)).astype(BF16)
            left_b.start()

        def total():
            to_partner(3).wait_recv()
            for c in (right_a, right_b, left_a, left_b):
                c.wait_recv()
            mine = part[core, chip, u].astype(F32) + prec[chip, u].astype(F32)
            out = []
            for half in range(2):
                sl = slice(half * rows, (half + 1) * rows)
                out.append(mine[sl] + fin[half, u].astype(F32) + fin[2 + half, u].astype(F32))
            return out

        def drain():
            for o in range(4):
                to_partner(o).wait_send()
            for c in (opp_a, opp_b, right_a, right_b, left_a, left_b):
                c.wait_send()

        return to_partner, first, relay, total, drain

    rs1 = [scatter(part1, prec1, rel1, fin1, u, d1_send, d1_recv, r1_send, r1_recv) for u in range(2)]
    def project_out(u):
        o_u = obuf[u]
        for o in range(4):
            d = chips[o]
            res = jnp.dot(o_u, wo[:, pl.ds(pl.multiple_of(d * dchip, dchip), dchip)], preferred_element_type=F32).astype(BF16)
            for c in range(2):
                part1[c, d, u] = res[:, c * dblk:(c + 1) * dblk]
            rs1[u][0](o).start()

    my_cols = pl.ds(pl.multiple_of(me * dblk, 128), dblk)
    a2_a, a2_b, a2_arrive, a2_drain = gather(g2, a2_send, a2_recv)

    def hidden_rows(u):
        per = half_n // TL
        hb = []
        for half, sums in enumerate(rs1[u][3]()):
            xs = jnp.concatenate([g1[u * per + half * (per // 2) + i, :, my_cols] for i in range(per // 2)], axis=0)
            hid = (xs.astype(F32) + sums).astype(BF16)
            g2[own, u * half_n + half * (half_n // 2):u * half_n + (half + 1) * (half_n // 2), :] = hid
            h32 = hid.astype(F32)
            hb.append(jnp.sum(h32 * h32, axis=-1, keepdims=True))
        return hb

    with scope("att00"):
        vc_copy.wait()
        attend(0, 0)
    with scope("att01"):
        attend(0, 1)
    with scope("out0"):
        wo_copy.wait()
        project_out(0)
    with scope("att10"):
        attend(1, 0)
    with scope("rs10_first"):
        rs1[0][1]()
    with scope("att11"):
        attend(1, 1)
    with scope("out1"):
        project_out(1)
    with scope("rs10_relay"):
        rs1[0][2]()
    with scope("rs11_first"):
        rs1[1][1]()
    with scope("rs10_total"):
        ss = hidden_rows(0)
        for c in a2_a:
            c.start()
    with scope("rs11_relay"):
        rs1[1][2]()
    with scope("rs11_total"):
        ss = ss + hidden_rows(1)
        ssbuf[own] = jnp.broadcast_to(jnp.concatenate(ss, axis=0), (T, T)).T[0:8]

    def ss_copy(src, k):
        dev = lax.rem(me + k, n_dev)
        return pltpu.make_async_remote_copy(ssbuf.at[src], ssbuf.at[src], ss_send.at[k - 1], ss_recv.at[k - 1], device_id={"tp": dev}, device_id_type=MESH)

    for k in range(1, n_dev):
        ss_copy(own, k).start()
    for c in a2_b:
        c.start()
    with scope("caches"):
        k_out = new_cache(kc, kch_ref, kn_hbm, 4)
        v_out = new_cache(vc, vch_ref, vn_hbm, 5)
    with scope("ss_wait"):
        for k in range(1, n_dev):
            ss_copy(lax.rem(me + n_dev - k, n_dev), k).wait_recv()
    tot = ssbuf[0]
    for k in range(1, n_dev):
        tot = tot + ssbuf[k]
    inv_row = lax.rsqrt(tot[0:1] * (1.0 / D) + NORM_EPS)
    inv = jnp.broadcast_to(inv_row, (T, T)).T[:, 0:1]

    def gate_up(s):
        d = order[s]
        for c in range(2):
            b = 2 * d + c
            gain = jnp.concatenate([mgain[pl.ds(b * (dblk // HD) + i, 1), :] for i in range(dblk // HD)], axis=1)
            mbuf[:, c * dblk:(c + 1) * dblk] = (g2[b].astype(F32) * inv * gain).astype(BF16)
        gu_wait(s)
        for n in range(gu_n):
            part = jnp.dot(mbuf[...], arena[gu_base(s) + n * dchip:gu_base(s) + (n + 1) * dchip, :], preferred_element_type=F32)
            if s:
                part = acc[:, n * SLOT:(n + 1) * SLOT] + part
            acc[:, n * SLOT:(n + 1) * SLOT] = part

    with scope("a2_0"):
        a2_arrive(PMA)
        a2_arrive(LA)
        a2_arrive(RB)
        a2_arrive(PMB)
    with scope("gu0"):
        gate_up(0)
        wd_half = wd_sem.shape[0] // 2
        for j in range(wd_half):
            wd_copy(j).start()
    with scope("a2_1"):
        for s in (RA, LB, PLA, PLB):
            a2_arrive(s)
    with scope("gu1"):
        gate_up(1)
        for j in range(wd_half, 2 * wd_half):
            wd_copy(j).start()
    with scope("a2_2"):
        a2_arrive(OA)
        a2_arrive(OB)
        a2_arrive(PRA)
        a2_arrive(PRB)
    with scope("gu2"):
        gate_up(2)
    with scope("a2_3"):
        a2_arrive(POA)
        a2_arrive(POB)
    with scope("gu3"):
        gate_up(3)
    with scope("silu"):
        for c0 in range(0, F, 256):
            gate = acc[:, c0:c0 + 256]
            up = acc[:, F + c0:F + c0 + 256]
            ubuf[:, c0:c0 + 256] = (gate * (1.0 / (1.0 + jnp.exp(-gate))) * up).astype(BF16)

    n_q = D // Q_COLS
    per_q = Q_COLS // SLOT
    rs2 = [scatter(part2, prec2, rel2, fin2, q, d2_send, d2_recv, r2_send, r2_recv) for q in range(n_q)]

    def down(q):
        for jj in range(per_q):
            j = q * per_q + jj
            wd_copy(j).wait()
            res = jnp.dot(ubuf[...], arena[wd_base + j * F:wd_base + (j + 1) * F, :], preferred_element_type=F32).astype(BF16)
            for b in range(n_dev):
                part2[b % 2, b // 2, q, :, jj * SLOT:(jj + 1) * SLOT] = res[b * TL:(b + 1) * TL]
        for o in range(4):
            rs2[q][0](o).start()

    def finish(q):
        sums = jnp.concatenate(rs2[q][3](), axis=0)
        tok = pl.ds(pl.multiple_of(me * TL, TL), TL)
        for k in range(Q_COLS // HD):
            at = q * Q_COLS + k * HD
            hid = g2[at // dblk, tok, at % dblk:at % dblk + HD]
            xout_ref[:, at:at + HD] = (hid.astype(F32) + sums[:, k * HD:(k + 1) * HD]).astype(BF16)

    for q in range(n_q + 2):
        if q < n_q:
            with scope(f"down{q}"):
                down(q)
        if 0 <= q - 1 < n_q:
            with scope(f"rs2{q - 1}_first"):
                rs2[q - 1][1]()
        if 0 <= q - 2 < n_q:
            with scope(f"rs2{q - 2}_relay"):
                rs2[q - 2][2]()
    for q in range(n_q):
        with scope(f"rs2{q}_total"):
            finish(q)

    a1_drain()
    a2_drain()
    for k in range(1, n_dev):
        ss_copy(own, k).wait_send()
    for r in rs1 + rs2:
        r[4]()
    k_out.wait()
    v_out.wait()


def solution(mesh):
    row_spec = P('dp', 'tp', None)
    cache_spec = P('dp', None, 'tp', None)
    head_cols = P(None, 'tp', None)
    in_specs = (row_spec, P('dp'), cache_spec, cache_spec, P(), head_cols, head_cols, head_cols, P('tp', None, None), P(), P(None, 'tp'), P(None, 'tp'), P('tp', None))
    out_specs = (row_spec, cache_spec, cache_spec)
    n_dev = mesh.shape['tp']

    def local_layer(x_in, start_pos, k_cache, v_cache, attn_gain, w_query, w_key, w_value, w_out, mlp_gain, w_gate, w_up, w_down):
        _, TL, D = x_in.shape
        W, HD = k_cache.shape[1], k_cache.shape[3]
        G = w_query.shape[1]
        F = w_gate.shape[1]
        T = TL * n_dev
        n_chip = n_dev // 2
        dblk, dchip = D // n_dev, D // n_chip
        inv_freq = np.repeat(np.power(ROPE_BASE, -np.arange(0, HD, 2) / HD), 2).astype(np.float32)
        vmem = pl.BlockSpec(memory_space=pltpu.VMEM)
        hbm = pl.BlockSpec(memory_space=pl.ANY)
        smem = pl.BlockSpec(memory_space=pltpu.SMEM)
        gu_n = 2 * F // SLOT
        V = pltpu.VMEM
        dma = pltpu.SemaphoreType.DMA
        half = T // 2
        n_q = D // Q_COLS
        scratch = [
            V((n_dev, TL, D), BF16), V((n_dev, T, dblk), BF16), V((T, D), BF16), V((T, dchip), BF16),
            V((2, n_chip, 2, half, dblk), BF16), V((2, n_chip, n_q, TL, Q_COLS), BF16),
            V((n_chip, 2, half, dblk), BF16), V((n_chip, n_q, TL, Q_COLS), BF16),
            V((2, 2, half // 2, dblk), BF16), V((2, n_q, TL // 2, Q_COLS), BF16),
            V((4, 2, half // 2, dblk), BF16), V((4, n_q, TL // 2, Q_COLS), BF16),
            V((n_dev, 8, T), F32),
            V((n_chip * gu_n * dchip, SLOT), BF16), V((G * HD, D), BF16), V((512, HD), F32),
            V((HD, W), BF16), V((W, HD), BF16), V((W, HD), BF16),
            V((2, G * half, HD), BF16), V((2 * half, W), F32), V((2, half, G * HD), BF16),
            V((T, 2 * F), F32), V((T, F), BF16), V((T, HD), BF16), V((T, HD), BF16), V((D // HD, HD), F32), V((D // HD, HD), F32), V((T, HD), F32), V((T, HD), F32),
            dma((6,)), dma((SLOT // HD,)), dma((4,)), dma((n_chip,)), dma((D // SLOT,)),
            dma((14,)), dma((14,)), dma((14,)), dma((14,)), dma((n_dev - 1,)), dma((n_dev - 1,)),
            dma((2, 4)), dma((2, 4)), dma((n_q, 4)), dma((n_q, 4)),
            dma((2, 6)), dma((2, 6)), dma((n_q, 6)), dma((n_q, 6)),
        ]
        x_out, k_new, v_new = pl.pallas_call(
            functools.partial(layer_kernel, n_dev, (D, T, TL, HD, F, W, G)),
            out_shape=[jax.ShapeDtypeStruct((TL, D), BF16), jax.ShapeDtypeStruct((W, HD), BF16), jax.ShapeDtypeStruct((W, HD), BF16)],
            in_specs=[smem, hbm, hbm, hbm, vmem, hbm, hbm, hbm, hbm, vmem, hbm, hbm, hbm, vmem],
            out_specs=[vmem, hbm, hbm],
            scratch_shapes=scratch,
            compiler_params=pltpu.CompilerParams(collective_id=0, has_side_effects=True, vmem_limit_bytes=67043328),
            name="layer",
        )(
            start_pos, x_in[0], k_cache.reshape(W, HD), v_cache.reshape(W, HD), attn_gain.reshape(D // HD, HD),
            w_query.reshape(D * G, HD), w_key.reshape(D, HD), w_value.reshape(D, HD), w_out.reshape(G * HD, D),
            mlp_gain.reshape(D // HD, HD), w_gate, w_up, w_down, inv_freq[None, :],
        )
        return x_out[None], k_new.reshape(k_cache.shape), v_new.reshape(v_cache.shape)

    return jax.shard_map(local_layer, mesh=mesh, in_specs=in_specs, out_specs=out_specs, check_vma=False)
```
